16 devices in a mesh: dp: 4 (over y, z, core), tp: 4 (over x).
Axes of the slice: x: 4, y: 2, z: 1, core: 2. Of those that a mesh axis runs over, the one named last changes fastest.
The devices are a block of a 4x4x4 slice.
Arguments:
- x: bfloat16 [256, 3072], P('dp'), parts along dimension 0
- k_cache: bfloat16 [256, 1024, 32, 96], P('dp', None, 'tp'), parts along dimension 0
- v_cache: bfloat16 [256, 1024, 32, 96], P('dp', None, 'tp'), parts along dimension 0
- gain_a: bfloat16 [3072], replicated
- wq: bfloat16 [3072, 3072], P(None, 'tp')
- wo: bfloat16 [3072, 3072], P('tp')
- gain_m: bfloat16 [3072], replicated
- w_gate: bfloat16 [3072, 8192], P(None, 'tp')
- w_up: bfloat16 [3072, 8192], P(None, 'tp')
- w_down: bfloat16 [8192, 3072], P('tp')
Outputs:
- output: bfloat16 [256, 3072], P('dp'), parts along dimension 0
There are 4 independent parts. The reference program is written for one: setup_inputs(seed, part) draws one part's arguments, and reference() takes and returns one part's arrays. A program takes and returns all parts, laid end to end along the dimension named above; an argument that names none is the same for every part.
All inputs are finite; a program needn't handle non-finite values.
Results may differ from the reference program's by a relative error of at most 0.017.
Values are sent between devices in bfloat16 or wider.
A program may use at most 1.5 GiB of HBM per device.

```python
import jax
import jax.numpy as jnp
from jax import lax

BATCH = 64
CACHE = 1024
D = 3072
HEADS = 32
KV_HEADS = 32
HEAD = 96
FF = 8192
THETA = 10000


def setup_inputs(seed: int = 0, part: int = 0) -> dict:
    kx, kc, kw, kn, kq, ko, km, kg, ku, kd = jax.random.split(jax.random.key(seed), 10)
    kx, kc, kw = (jax.random.fold_in(k, part) for k in (kx, kc, kw))

    def weights(key, rows, columns):
        return jax.random.normal(key, (rows, columns), jnp.float32) * rows**-0.5

    drawn = {
        "x": jax.random.normal(kx, (BATCH, D), jnp.float32),
        "k_cache": 2 * jax.random.normal(kc, (BATCH, CACHE, KV_HEADS, HEAD), jnp.float32),
        "v_cache": 4 * jax.random.normal(kw, (BATCH, CACHE, KV_HEADS, HEAD), jnp.float32),
        "gain_a": 1 + 0.1 * jax.random.normal(kn, (D,), jnp.float32),
        "wq": 2 * weights(kq, D, HEADS * HEAD),
        "wo": weights(ko, HEADS * HEAD, D),
        "gain_m": 1 + 0.1 * jax.random.normal(km, (D,), jnp.float32),
        "w_gate": weights(kg, D, FF),
        "w_up": weights(ku, D, FF),
        "w_down": 2 * weights(kd, FF, D),
    }
    return {k: v.astype(jnp.bfloat16) for k, v in drawn.items()}


def normed(x, gain):
    wide = x.astype(jnp.float32)
    scale = lax.rsqrt(jnp.mean(wide * wide, -1, keepdims=True) + 1e-6)
    return (wide * scale * gain.astype(jnp.float32)).astype(jnp.bfloat16)


def turned(t, place, theta):
    half = t.shape[-1] // 2
    angle = place.astype(jnp.float32)[:, None] * theta ** (-jnp.arange(half, dtype=jnp.float32) / half)
    cos, sin = jnp.cos(angle)[:, None], jnp.sin(angle)[:, None]
    a, b = t[..., :half].astype(jnp.float32), t[..., half:].astype(jnp.float32)
    return jnp.concatenate([a * cos - b * sin, b * cos + a * sin], -1).astype(jnp.bfloat16)


def matmul(a, w):
    return jnp.dot(a, w, preferred_element_type=jnp.float32).astype(jnp.bfloat16)


def einsum(form, a, b):
    return jnp.einsum(form, a.astype(jnp.float32), b.astype(jnp.float32))


def seen_by(a, wq, k_cache, v_cache, head, theta):
    batch, cache, kv_heads = k_cache.shape[:3]
    place = jnp.full((batch,), cache - 1)
    q = turned(matmul(a, wq).reshape(batch, -1, head), place, theta).reshape(batch, kv_heads, -1, head)
    scores = einsum("bgsd,bugd->bgsu", q, k_cache) * head**-0.5
    weights = jax.nn.softmax(scores, -1).astype(jnp.bfloat16)
    return einsum("bgsu,bugd->bgsd", weights, v_cache).astype(jnp.bfloat16).reshape(batch, -1)


def hidden_of(b, w_gate, w_up):
    gate = jnp.dot(b, w_gate, preferred_element_type=jnp.float32)
    up = jnp.dot(b, w_up, preferred_element_type=jnp.float32)
    return (jax.nn.silu(gate) * up).astype(jnp.bfloat16)


def reference(x, k_cache, v_cache, gain_a, wq, wo, gain_m, w_gate, w_up, w_down):
    seen = seen_by(normed(x, gain_a), wq, k_cache, v_cache, HEAD, THETA)
    h = (x.astype(jnp.float32) + jnp.dot(seen, wo, preferred_element_type=jnp.float32)).astype(jnp.bfloat16)
    hidden = hidden_of(normed(h, gain_m), w_gate, w_up)
    return (h.astype(jnp.float32) + jnp.dot(hidden, w_down, preferred_element_type=jnp.float32)).astype(jnp.bfloat16)
```

```python
import functools

import jax
import jax.numpy as jnp
import numpy as np
from jax import lax
from jax.experimental import pallas as pl
from jax.experimental.pallas import tpu as pltpu
from jax.sharding import PartitionSpec as P

HEAD = 96
THETA = 10000
MESH = pl.DeviceIdType.MESH
F32, BF16 = jnp.float32, jnp.bfloat16
PAIR = 2
RING = 3
COLS = 512
EARLY = 48
VMEM_BYTES = 67_043_328


def dot(a, b):
    return lax.dot_general(a, b, (((1,), (0,)), ((), ())), preferred_element_type=F32)


def dot_t(a, b):
    return lax.dot_general(a, b, (((1,), (1,)), ((), ())), preferred_element_type=F32)


def kernel(n, x_hbm, k_hbm, v_hbm, ga_hbm, gm_hbm, turn_hbm, wq_hbm, wo_hbm, wg_hbm, wu_hbm, wd_hbm, out,
           xv, gav, gmv, turnv, gv, uv, dv, wov, kbuf, vbuf, q_s, s_s, seen, normed, hbuf, hidden,
           acc, t1, rs1, t2, rs2, ybuf,
           sem_in, sem_k, sem_v, sem_w, sem_d, send1, recv1, gsend1, grecv1, send2, recv2, gsend2, grecv2):
    batch, d = xv.shape
    width = d // n
    inner = q_s.shape[1]
    heads = inner // HEAD
    rows = PAIR * heads
    steps = batch // PAIR
    chunks = gv.shape[0]
    me = lax.axis_index("tp")

    def peer(j):
        return lax.rem(me + j, n)

    def block_of(j):
        return pl.ds(pl.multiple_of(peer(j) * width, width), width)

    copy = pltpu.make_async_copy
    x_in = copy(x_hbm, xv, sem_in.at[0])
    ga_in = copy(ga_hbm, gav, sem_in.at[1])
    gm_in = copy(gm_hbm, gmv, sem_in.at[2])
    turn_in = copy(turn_hbm, turnv, sem_in.at[3])
    wq_ins = []
    for c in range(0, inner, COLS):
        size = min(COLS, inner - c)
        wq_ins.append((c, size, copy(wq_hbm.at[:, pl.ds(c, size)], gv.at[c // COLS, :, pl.ds(0, size)], sem_w.at[0, c // COLS])))
    wo_in = copy(wo_hbm, wov, sem_in.at[4])

    def k_in(p):
        slot = lax.rem(p, RING)
        return copy(k_hbm.at[pl.ds(p * PAIR, PAIR)], kbuf.at[slot], sem_k.at[slot])

    def v_in(p):
        slot = lax.rem(p, RING)
        return copy(v_hbm.at[pl.ds(p * PAIR, PAIR)], vbuf.at[slot], sem_v.at[slot])

    def gate_in(c):
        return copy(wg_hbm.at[:, pl.ds(pl.multiple_of(c * COLS, COLS), COLS)], gv.at[c], sem_w.at[0, c])

    def up_in(c):
        return copy(wu_hbm.at[:, pl.ds(pl.multiple_of(c * COLS, COLS), COLS)], uv.at[c], sem_w.at[1, c])

    def down_in(j):
        return copy(wd_hbm.at[:, block_of(j)], dv.at[j], sem_d.at[j])

    x_in.start()
    ga_in.start()
    turn_in.start()
    for _, _, c in wq_ins:
        c.start()
    gm_in.start()
    for p in range(RING):
        k_in(p).start()
        v_in(p).start()
    wo_in.start()

    barrier = pltpu.get_barrier_semaphore()
    for j in range(1, n):
        pl.semaphore_signal(barrier, inc=1, device_id={"tp": peer(j)}, device_id_type=MESH)
    pl.semaphore_wait(barrier, n - 1)

    def norm_rows(parts, gain, r, many):
        wide = [part(r, many).astype(F32) for part in parts]
        total = sum(jnp.sum(w * w, -1, keepdims=True) for w in wide)
        scale = lax.rsqrt(total / d + 1e-6)
        step = d // len(parts)
        for i, w in enumerate(wide):
            at = pl.ds(i * step, step)
            normed[pl.ds(r, many), at] = (w * scale * gain[:, at].astype(F32)).astype(BF16)

    x_in.wait()
    ga_in.wait()
    for r in range(0, batch, 16):
        norm_rows([lambda r, many: xv[pl.ds(r, many), :]], gav, r, 16)
    turn_in.wait()
    for c, size, c_in in wq_ins:
        c_in.wait()
        q_s[:, pl.ds(c, size)] = dot(normed[...], gv[c // COLS, :, pl.ds(0, size)])
    half = HEAD // 2
    lane = lax.broadcasted_iota(jnp.int32, (16, inner), 1)
    first = lax.rem(lane, HEAD) < half
    for r in range(0, batch, 16):
        q = q_s[pl.ds(r, 16), :].astype(BF16).astype(F32)
        other = jnp.where(first, pltpu.roll(q, inner - half, 1), pltpu.roll(q, half, 1))
        q_s[pl.ds(r, 16), :] = q * turnv[pl.ds(0, 1), :] + other * turnv[pl.ds(1, 1), :]

    row = lax.broadcasted_iota(jnp.int32, (rows, inner), 0)
    mine = lax.broadcasted_iota(jnp.int32, (rows, inner), 1) // HEAD == lax.rem(row, heads)

    def scores(p):
        slot = lax.rem(p, RING)
        q = jnp.concatenate(
            [jnp.broadcast_to(q_s[pl.ds(p * PAIR + i, 1), :], (heads, inner)) for i in range(PAIR)], 0
        )
        q = jnp.where(mine, q, 0.0).astype(BF16)
        for i in range(PAIR):
            at = pl.ds(i * heads, heads)
            s_s[at, :] = dot(q, kbuf[slot, i])[i * heads : (i + 1) * heads]

    def attend(p, last):
        v_in(p).wait()
        if not last:
            k_in(p + 1).wait()
        s = s_s[...] * HEAD**-0.5
        e = jnp.exp(s - jnp.max(s, -1, keepdims=True))
        w = (e * (1.0 / jnp.sum(e, -1, keepdims=True))).astype(BF16)
        if not last:
            scores(p + 1)
        slot = lax.rem(p, RING)
        for i in range(PAIR):
            o = dot_t(w, vbuf[slot, i])[i * heads : (i + 1) * heads]
            seen[pl.ds(p * PAIR + i, 1), :] = jnp.sum(
                jnp.where(mine[i * heads : (i + 1) * heads], o, 0.0), 0, keepdims=True
            )

        if not last:
            @pl.when(p + 1 + RING < steps)
            def _():
                k_in(p + 1 + RING).start()

            @pl.when(p + RING < steps)
            def _():
                v_in(p + RING).start()

    order = [2, 1, 3] if n == 4 else list(range(1, n))

    def terms_out(part, r, many):
        at = pl.ds(r, many)
        a = seen[at, :].astype(BF16)
        sent = []
        for j in order:
            t1[j - 1, at, :] = dot(a, wov[:, block_of(j)]).astype(BF16)
            c = pltpu.make_async_remote_copy(
                t1.at[j - 1, at], rs1.at[j - 1, at], send1.at[part, j - 1], recv1.at[part, j - 1],
                device_id={"tp": peer(j)}, device_id_type=MESH,
            )
            c.start()
            sent.append(c)
        acc[at, :] = dot(a, wov[:, block_of(0)])
        return sent

    def states_out(part, r, many, arrived):
        at = pl.ds(r, many)
        for c in arrived:
            c.wait_recv()
        total = acc[at, :]
        for j in range(1, n):
            total = total + rs1[j - 1, at, :].astype(F32)
        hbuf[me, at, :] = (xv[at, block_of(0)].astype(F32) + total).astype(BF16)
        sent = []
        for j in order:
            c = pltpu.make_async_remote_copy(
                hbuf.at[me, at], hbuf.at[me, at], gsend1.at[part, j - 1], grecv1.at[part, j - 1],
                device_id={"tp": peer(j)}, device_id_type=MESH,
            )
            c.start()
            sent.append(c)
        return sent

    def attend_all(lo, hi):
        def body(p, carry):
            attend(p, False)
            return carry

        lax.fori_loop(lo, hi, body, 0)

    k_in(0).wait()
    scores(0)
    k_in(RING).start()
    early_steps = EARLY // PAIR
    between = early_steps + (steps - early_steps) // 2
    attend_all(0, early_steps)
    wo_in.wait()
    out_a = terms_out(0, 0, EARLY)
    attend_all(early_steps, between)
    all_a = states_out(0, 0, EARLY, out_a)
    attend_all(between, steps - RING)
    for c in range(chunks):
        gate_in(c).start()
        up_in(c).start()
    for j in order + [0]:
        down_in(j).start()
    attend_all(steps - RING, steps - 1)
    attend(steps - 1, True)
    out_b = terms_out(1, EARLY, batch - EARLY)
    all_b = states_out(1, EARLY, batch - EARLY, out_b)
    for c in all_a + all_b:
        c.wait_recv()

    gm_in.wait()
    for r in range(0, batch, 16):
        norm_rows([lambda r, many, i=i: hbuf[i, pl.ds(r, many), :] for i in range(n)], gmv, r, 16)

    def hidden_step(c, carry):
        gate_in(c).wait()
        up_in(c).wait()
        g = dot(normed[...], gv[c])
        u = dot(normed[...], uv[c])
        hidden[:, pl.ds(pl.multiple_of(c * COLS, COLS), COLS)] = (jax.nn.silu(g) * u).astype(BF16)
        return carry

    lax.fori_loop(0, chunks, hidden_step, 0)
    sent2 = []
    for j in order:
        down_in(j).wait()
        t2[j - 1] = dot(hidden[...], dv[j]).astype(BF16)
        c = pltpu.make_async_remote_copy(
            t2.at[j - 1], rs2.at[j - 1], send2.at[j - 1], recv2.at[j - 1],
            device_id={"tp": peer(j)}, device_id_type=MESH,
        )
        c.start()
        sent2.append(c)
    down_in(0).wait()
    total = dot(hidden[...], dv[0])
    acc[...] = total
    for c in sent2:
        c.wait_recv()
    total = acc[...]
    for j in range(1, n):
        total = total + rs2[j - 1].astype(F32)
    ybuf[me] = (hbuf[me].astype(F32) + total).astype(BF16)
    all_y = []
    for j in order:
        c = pltpu.make_async_remote_copy(
            ybuf.at[me], ybuf.at[me], gsend2.at[j - 1], grecv2.at[j - 1],
            device_id={"tp": peer(j)}, device_id_type=MESH,
        )
        c.start()
        all_y.append(c)
    for c in all_y:
        c.wait_recv()
    for i in range(n):
        out[:, pl.ds(i * width, width)] = ybuf[i]
    for c in out_a + out_b + all_a + all_b + sent2 + all_y:
        c.wait_send()


def turns(place, inner):
    half = HEAD // 2
    angle = np.float32(place) * np.float32(THETA) ** (-np.arange(half, dtype=np.float32) / np.float32(half))
    cos, sin = np.cos(angle.astype(np.float32)), np.sin(angle.astype(np.float32))
    one = np.stack([np.concatenate([cos, cos]), np.concatenate([-sin, sin])])
    return np.tile(one, (1, inner // HEAD)).astype(np.float32)


def solution(mesh):
    n = mesh.shape["tp"]

    def step(x, k_cache, v_cache, gain_a, wq, wo, gain_m, w_gate, w_up, w_down):
        batch, d = x.shape
        places, heads, head = k_cache.shape[1:]
        inner, ff = heads * head, w_gate.shape[1]
        width = d // n
        turn = jnp.asarray(turns(places - 1, inner))

        def rows_first(c):
            return jnp.transpose(c, (0, 2, 3, 1)).reshape(batch, inner, places)

        anywhere = pl.BlockSpec(memory_space=pl.ANY)
        dma = pltpu.SemaphoreType.DMA
        moved = n - 1
        return pl.pallas_call(
            functools.partial(kernel, n),
            name="layer",
            out_shape=jax.ShapeDtypeStruct((batch, d), BF16),
            in_specs=[anywhere] * 11,
            out_specs=pl.BlockSpec(memory_space=pltpu.VMEM),
            scratch_shapes=[
                pltpu.VMEM((batch, d), BF16),
                pltpu.VMEM((1, d), BF16),
                pltpu.VMEM((1, d), BF16),
                pltpu.VMEM((2, inner), F32),
                pltpu.VMEM((ff // COLS, d, COLS), BF16),
                pltpu.VMEM((ff // COLS, d, COLS), BF16),
                pltpu.VMEM((n, ff, width), BF16),
                pltpu.VMEM((inner, d), BF16),
                pltpu.VMEM((RING, PAIR, inner, places), BF16),
                pltpu.VMEM((RING, PAIR, inner, places), BF16),
                pltpu.VMEM((batch, inner), F32),
                pltpu.VMEM((PAIR * heads, places), F32),
                pltpu.VMEM((batch, inner), F32),
                pltpu.VMEM((batch, d), BF16),
                pltpu.VMEM((n, batch, width), BF16),
                pltpu.VMEM((batch, ff), BF16),
                pltpu.VMEM((batch, width), F32),
                pltpu.VMEM((moved, batch, width), BF16),
                pltpu.VMEM((moved, batch, width), BF16),
                pltpu.VMEM((moved, batch, width), BF16),
                pltpu.VMEM((moved, batch, width), BF16),
                pltpu.VMEM((n, batch, width), BF16),
                dma((5,)),
                dma((RING,)),
                dma((RING,)),
                dma((2, ff // COLS)),
                dma((n,)),
            ]
            + [dma((2, moved))] * 4
            + [dma((moved,))] * 4,
            compiler_params=pltpu.CompilerParams(
                collective_id=0, has_side_effects=True, vmem_limit_bytes=VMEM_BYTES
            ),
        )(
            x, rows_first(k_cache), rows_first(v_cache), gain_a.reshape(1, d), gain_m.reshape(1, d), turn,
            wq, wo, w_gate, w_up, w_down,
        )

    states, cache, columns, rows_of = P("dp", None), P("dp", None, "tp", None), P(None, "tp"), P("tp", None)
    return jax.shard_map(
        step,
        mesh=mesh,
        in_specs=(states, cache, cache, P(None), columns, rows_of, P(None), columns, columns, rows_of),
        out_specs=states,
        check_vma=False,
    )
```

```python
import functools

import jax
import jax.numpy as jnp
import numpy as np
from jax import lax
from jax.experimental import pallas as pl
from jax.experimental.pallas import tpu as pltpu
from jax.sharding import PartitionSpec as P

HEAD = 96
THETA = 10000
MESH = pl.DeviceIdType.MESH
F32, BF16 = jnp.float32, jnp.bfloat16
PAIR = 2
RING = 3
COLS = 512
EARLY = 48
VMEM_BYTES = 66_400_000


def dot(a, b):
    return lax.dot_general(a, b, (((1,), (0,)), ((), ())), preferred_element_type=F32)


def dot_t(a, b):
    return lax.dot_general(a, b, (((1,), (1,)), ((), ())), preferred_element_type=F32)


def kernel(n, x_hbm, k_hbm, v_hbm, ga_hbm, gm_hbm, turn_hbm, wq_hbm, wo_hbm, wg_hbm, wu_hbm, wd_hbm, out,
           xv, gav, gmv, gaf, gmf, turnv, gv, uv, dv, wov, kbuf, vbuf, q_s, s_s, seen, normed, hbuf, hidden,
           acc, t1, rs1, t2, rs2, ybuf,
           sem_in, sem_k, sem_v, sem_w, sem_d, send1, recv1, gsend1, grecv1, send2, recv2, gsend2, grecv2):
    batch, d = xv.shape
    width = d // n
    inner = q_s.shape[1]
    heads = inner // HEAD
    rows = PAIR * heads
    steps = batch // PAIR
    chunks = gv.shape[0]
    me = lax.axis_index("tp")

    def peer(j):
        return lax.rem(me + j, n)

    def block_of(j):
        return pl.ds(pl.multiple_of(peer(j) * width, width), width)

    copy = pltpu.make_async_copy
    x_in = copy(x_hbm, xv, sem_in.at[0])
    ga_in = copy(ga_hbm, gav, sem_in.at[1])
    gm_in = copy(gm_hbm, gmv, sem_in.at[2])
    turn_in = copy(turn_hbm, turnv, sem_in.at[3])
    wq_ins = []
    for c in range(0, inner, COLS):
        size = min(COLS, inner - c)
        wq_ins.append((c, size, copy(wq_hbm.at[:, pl.ds(c, size)], gv.at[c // COLS, :, pl.ds(0, size)], sem_w.at[0, c // COLS])))
    wo_in = copy(wo_hbm, wov, sem_in.at[4])

    def k_in(p):
        slot = lax.rem(p, RING)
        return copy(k_hbm.at[pl.ds(p * PAIR, PAIR)], kbuf.at[slot], sem_k.at[slot])

    def v_in(p):
        slot = lax.rem(p, RING)
        return copy(v_hbm.at[pl.ds(p * PAIR, PAIR)], vbuf.at[slot], sem_v.at[slot])

    def gate_in(c):
        return copy(wg_hbm.at[:, pl.ds(pl.multiple_of(c * COLS, COLS), COLS)], gv.at[c], sem_w.at[0, c])

    def up_in(c):
        return copy(wu_hbm.at[:, pl.ds(pl.multiple_of(c * COLS, COLS), COLS)], uv.at[c], sem_w.at[1, c])

    def down_in(j):
        return copy(wd_hbm.at[:, block_of(j)], dv.at[j], sem_d.at[j])

    x_in.start()
    ga_in.start()
    turn_in.start()
    for _, _, c in wq_ins:
        c.start()
    gm_in.start()
    for p in range(RING):
        k_in(p).start()
        v_in(p).start()
    wo_in.start()

    with jax.named_scope("entry"):
        barrier = pltpu.get_barrier_semaphore()
        for j in range(1, n):
            pl.semaphore_signal(barrier, inc=1, device_id={"tp": peer(j)}, device_id_type=MESH)
        pl.semaphore_wait(barrier, n - 1)

    def widened(gain):
        g = gain[...].astype(F32)
        return jnp.concatenate([g[i : i + 1] for i in range(d // 128)], 1)

    def norm_rows(parts, gain, r, many):
        wide = [part(r, many).astype(F32) for part in parts]
        total = sum(jnp.sum(w * w, -1, keepdims=True) for w in wide)
        scale = lax.rsqrt(total / d + 1e-6)
        step = d // len(parts)
        for i, w in enumerate(wide):
            at = pl.ds(i * step, step)
            normed[pl.ds(r, many), at] = (w * scale * gain[:, at]).astype(BF16)

    with jax.named_scope("x_wait"):
        x_in.wait()
        ga_in.wait()
    gaf[...] = widened(gav)
    for r in range(0, batch, 16):
        norm_rows([lambda r, many: xv[pl.ds(r, many), :]], gaf, r, 16)
    turn_in.wait()
    for c, size, c_in in wq_ins:
        with jax.named_scope("wq_wait"):
            c_in.wait()
        q_s[:, pl.ds(c, size)] = dot(normed[...], gv[c // COLS, :, pl.ds(0, size)])
    half = HEAD // 2
    lane = lax.broadcasted_iota(jnp.int32, (16, inner), 1)
    first = lax.rem(lane, HEAD) < half
    for r in range(0, batch, 16):
        q = q_s[pl.ds(r, 16), :].astype(BF16).astype(F32)
        other = jnp.where(first, pltpu.roll(q, inner - half, 1), pltpu.roll(q, half, 1))
        q_s[pl.ds(r, 16), :] = q * turnv[pl.ds(0, 1), :] + other * turnv[pl.ds(1, 1), :]

    row = lax.broadcasted_iota(jnp.int32, (rows, inner), 0)
    mine = lax.broadcasted_iota(jnp.int32, (rows, inner), 1) // HEAD == lax.rem(row, heads)

    def scores(p):
        slot = lax.rem(p, RING)
        q = jnp.concatenate(
            [jnp.broadcast_to(q_s[pl.ds(p * PAIR + i, 1), :], (heads, inner)) for i in range(PAIR)], 0
        )
        q = jnp.where(mine, q, 0.0).astype(BF16)
        for i in range(PAIR):
            at = pl.ds(i * heads, heads)
            s_s[at, :] = dot(q, kbuf[slot, i])[i * heads : (i + 1) * heads]

    def attend(p, last):
        v_in(p).wait()
        if not last:
            k_in(p + 1).wait()
        s = s_s[...] * HEAD**-0.5
        e = jnp.exp(s - jnp.max(s, -1, keepdims=True))
        w = (e * (1.0 / jnp.sum(e, -1, keepdims=True))).astype(BF16)
        if not last:
            scores(p + 1)
        slot = lax.rem(p, RING)
        for i in range(PAIR):
            o = dot_t(w, vbuf[slot, i])[i * heads : (i + 1) * heads]
            seen[pl.ds(p * PAIR + i, 1), :] = jnp.sum(
                jnp.where(mine[i * heads : (i + 1) * heads], o, 0.0), 0, keepdims=True
            )

        if not last:
            @pl.when(p + 1 + RING < steps)
            def _():
                k_in(p + 1 + RING).start()

            @pl.when(p + RING < steps)
            def _():
                v_in(p + RING).start()

    order = [2, 1, 3] if n == 4 else list(range(1, n))
    places = order + [0]
    by_two = [places[i : i + 2] for i in range(0, n, 2)]
    parts = [(0, EARLY), (EARLY, batch - EARLY)]
    halves = [(i * (batch // 2), batch // 2) for i in range(2)]

    def to(j, src, dst, sems, k):
        return pltpu.make_async_remote_copy(
            src, dst, sems[0].at[k, j - 1], sems[1].at[k, j - 1], device_id={"tp": peer(j)}, device_id_type=MESH
        )

    def term1(k, j):
        at = pl.ds(*parts[k])
        return to(j, t1.at[j - 1, at], rs1.at[j - 1, at], (send1, recv1), k)

    def state1(k, j):
        at = pl.ds(*parts[k])
        return to(j, hbuf.at[me, at], hbuf.at[me, at], (gsend1, grecv1), k)

    def term2(k, j):
        at = pl.ds(*halves[k])
        return to(j, t2.at[j - 1, at], rs2.at[j - 1, at], (send2, recv2), k)

    def state2(k, j):
        at = pl.ds(*halves[k])
        return to(j, ybuf.at[me, at], ybuf.at[me, at], (gsend2, grecv2), k)

    def terms_out(k):
        at = pl.ds(*parts[k])
        a = seen[at, :].astype(BF16)
        for group in by_two:
            found = [dot(a, wov[:, block_of(j)]) for j in group]
            for j, t in zip(group, found):
                if j:
                    t1[j - 1, at, :] = t.astype(BF16)
                else:
                    acc[at, :] = t
            for j in group:
                if j:
                    term1(k, j).start()

    def states_out(k):
        at = pl.ds(*parts[k])
        for j in order:
            term1(k, j).wait_recv()
        total = acc[at, :]
        for j in range(1, n):
            total = total + rs1[j - 1, at, :].astype(F32)
        hbuf[me, at, :] = (xv[at, block_of(0)].astype(F32) + total).astype(BF16)
        for j in order:
            state1(k, j).start()

    def states_in(k):
        for j in order:
            state1(k, j).wait_recv()
        r, many = parts[k]
        for i in range(r, r + many, 16):
            norm_rows([lambda r, many, s=s: hbuf[s, pl.ds(r, many), :] for s in range(n)], gmf, i, 16)

    early_steps = EARLY // PAIR
    late = (steps - early_steps) // 4
    scope = jax.named_scope

    def body(p, carry):
        @pl.when(p == early_steps)
        def _():
            with scope("terms_a"):
                wo_in.wait()
                terms_out(0)

        @pl.when(p == early_steps + 2 * late)
        def _():
            with scope("states_a"):
                states_out(0)

        @pl.when(p == early_steps + 3 * late)
        def _():
            with scope("norm_a"):
                gm_in.wait()
                gmf[...] = widened(gmv)
                states_in(0)

        attend(p, False)

        @pl.when(p == steps - 1 - RING)
        def _():
            for c in range(chunks):
                gate_in(c).start(priority=1)
                up_in(c).start(priority=1)
            for j in places:
                down_in(j).start(priority=1)

        return carry

    with scope("first_scores"):
        k_in(0).wait()
        scores(0)
        k_in(RING).start()
    with scope("attend"):
        lax.fori_loop(0, steps - 1, body, 0)
    with scope("attend_last"):
        attend(steps - 1, True)
    with scope("terms_b"):
        terms_out(1)

    def hidden_out(c, rows):
        at = pl.ds(*rows)
        g = dot(normed[at, :], gv[c])
        u = dot(normed[at, :], uv[c])
        hidden[at, pl.ds(c * COLS, COLS)] = (jax.nn.silu(g) * u).astype(BF16)

    for c in range(chunks):
        if c == chunks // 2:
            with scope("states_b"):
                states_out(1)
        if c == chunks - 1:
            with scope("norm_b"):
                states_in(1)
        with scope("weights_wait"):
            gate_in(c).wait()
            up_in(c).wait()
        with scope("hidden_a"):
            hidden_out(c, (0, batch) if c == chunks - 1 else parts[0])
    with scope("hidden_b"):
        for c in range(chunks - 1):
            hidden_out(c, parts[1])
    for group in by_two:
        with scope("down_wait"):
            for j in group:
                down_in(j).wait()
        with scope("down"):
            found = [dot(hidden[...], dv[j]) for j in group]
            for j, t in zip(group, found):
                if j:
                    t2[j - 1] = t.astype(BF16)
                else:
                    acc[...] = t
        for k in range(2):
            for j in group:
                if j:
                    term2(k, j).start()
    for k in range(2):
        at = pl.ds(*halves[k])
        with scope("terms2_wait"):
            for j in order:
                term2(k, j).wait_recv()
        total = acc[at, :]
        for j in range(1, n):
            total = total + rs2[j - 1, at, :].astype(F32)
        ybuf[me, at, :] = (hbuf[me, at, :].astype(F32) + total).astype(BF16)
        for j in order:
            state2(k, j).start()
    with scope("states2_wait"):
        for k in range(2):
            for j in order:
                state2(k, j).wait_recv()
    for i in range(n):
        out[:, pl.ds(i * width, width)] = ybuf[i]
    for k in range(2):
        for j in order:
            for c in (term1, state1, term2, state2):
                c(k, j).wait_send()


def turns(place, inner):
    half = HEAD // 2
    angle = np.float32(place) * np.float32(THETA) ** (-np.arange(half, dtype=np.float32) / np.float32(half))
    cos, sin = np.cos(angle.astype(np.float32)), np.sin(angle.astype(np.float32))
    one = np.stack([np.concatenate([cos, cos]), np.concatenate([-sin, sin])])
    return np.tile(one, (1, inner // HEAD)).astype(np.float32)


def solution(mesh):
    n = mesh.shape["tp"]

    def step(x, k_cache, v_cache, gain_a, wq, wo, gain_m, w_gate, w_up, w_down):
        batch, d = x.shape
        places, heads, head = k_cache.shape[1:]
        inner, ff = heads * head, w_gate.shape[1]
        width = d // n
        turn = jnp.asarray(turns(places - 1, inner))

        def rows_first(c):
            return jnp.transpose(c, (0, 2, 3, 1)).reshape(batch, inner, places)

        anywhere = pl.BlockSpec(memory_space=pl.ANY)
        dma = pltpu.SemaphoreType.DMA
        moved = n - 1
        return pl.pallas_call(
            functools.partial(kernel, n),
            name="layer",
            out_shape=pltpu.VMEM((batch, d), BF16),
            in_specs=[anywhere] * 11,
            out_specs=pl.BlockSpec(memory_space=pltpu.VMEM),
            scratch_shapes=[
                pltpu.VMEM((batch, d), BF16),
                pltpu.VMEM((d // 128, 128), BF16),
                pltpu.VMEM((d // 128, 128), BF16),
                pltpu.VMEM((1, d), F32),
                pltpu.VMEM((1, d), F32),
                pltpu.VMEM((2, inner), F32),
                pltpu.VMEM((ff // COLS, d, COLS), BF16),
                pltpu.VMEM((ff // COLS, d, COLS), BF16),
                pltpu.VMEM((n, ff, width), BF16),
                pltpu.VMEM((inner, d), BF16),
                pltpu.VMEM((RING, PAIR, inner, places), BF16),
                pltpu.VMEM((RING, PAIR, inner, places), BF16),
                pltpu.VMEM((batch, inner), F32),
                pltpu.VMEM((PAIR * heads, places), F32),
                pltpu.VMEM((batch, inner), F32),
                pltpu.VMEM((batch, d), BF16),
                pltpu.VMEM((n, batch, width), BF16),
                pltpu.VMEM((batch, ff), BF16),
                pltpu.VMEM((batch, width), F32),
                pltpu.VMEM((moved, batch, width), BF16),
                pltpu.VMEM((moved, batch, width), BF16),
                pltpu.VMEM((moved, batch, width), BF16),
                pltpu.VMEM((moved, batch, width), BF16),
                pltpu.VMEM((n, batch, width), BF16),
                dma((5,)),
                dma((RING,)),
                dma((RING,)),
                dma((2, ff // COLS)),
                dma((n,)),
            ]
            + [dma((2, moved))] * 8,
            compiler_params=pltpu.CompilerParams(
                collective_id=0, has_side_effects=True, vmem_limit_bytes=VMEM_BYTES
            ),
        )(
            x, rows_first(k_cache), rows_first(v_cache), gain_a.reshape(-1, 128), gain_m.reshape(-1, 128), turn,
            wq, wo, w_gate, w_up, w_down,
        )

    states, cache, columns, rows_of = P("dp", None), P("dp", None, "tp", None), P(None, "tp"), P("tp", None)
    return jax.shard_map(
        step,
        mesh=mesh,
        in_specs=(states, cache, cache, P(None), columns, rows_of, P(None), columns, columns, rows_of),
        out_specs=states,
        check_vma=False,
    )
```

```python
import functools

import jax
import jax.numpy as jnp
import numpy as np
from jax import lax
from jax.experimental import pallas as pl
from jax.experimental.pallas import tpu as pltpu
from jax.sharding import PartitionSpec as P

HEAD = 96
THETA = 10000
MESH = pl.DeviceIdType.MESH
F32, BF16 = jnp.float32, jnp.bfloat16
PAIR = 2
RING = 3
COLS = 512
EARLY = 48
LATE = 8
VMEM_BYTES = 66_400_000


def dot(a, b):
    return lax.dot_general(a, b, (((1,), (0,)), ((), ())), preferred_element_type=F32)


def dot_t(a, b):
    return lax.dot_general(a, b, (((1,), (1,)), ((), ())), preferred_element_type=F32)


def kernel(n, shared, x_hbm, k_hbm, v_hbm, ga_hbm, gm_hbm, turn_hbm, wq_hbm, wo_hbm, wg_hbm, wu_hbm, wd_hbm, out,
           xv, gav, gmv, gaf, gmf, turnv, gv, uv, dv, wov, kbuf, vbuf, q_s, s_s, normed, hbuf, hidden,
           acc, t1, rs1, rs2, ybuf, tb, rb, hlate,
           sem_in, sem_k, sem_v, sem_w, sem_d, send1, recv1, gsend1, grecv1, send2, recv2, gsend2, grecv2, bsend, brecv, csend, crecv):
    batch, d = xv.shape
    t2 = t1
    seen = q_s
    width = d // n
    inner = q_s.shape[1]
    heads = inner // HEAD
    rows = PAIR * heads
    steps = batch // PAIR
    chunks = gv.shape[0]
    me = lax.axis_index("tp")

    def peer(j):
        return lax.rem(me + j, n)

    def block_of(j):
        return pl.ds(pl.multiple_of(peer(j) * width, width), width)

    copy = pltpu.make_async_copy
    x_in = copy(x_hbm, xv, sem_in.at[0])
    ga_in = copy(ga_hbm, gav, sem_in.at[1])
    gm_in = copy(gm_hbm, gmv, sem_in.at[2])
    turn_in = copy(turn_hbm, turnv, sem_in.at[3])
    wq_ins = []
    for c in range(0, inner, COLS):
        size = min(COLS, inner - c)
        wq_ins.append((c, size, copy(wq_hbm.at[:, pl.ds(c, size)], gv.at[c // COLS, :, pl.ds(0, size)], sem_w.at[0, c // COLS])))

    group = lax.axis_index("dp")
    core = lax.rem(group, 2)

    def half_of(many):
        return pl.ds(pl.multiple_of(core * (many // 2), many // 2), many // 2) if shared else pl.ds(0, many)

    def handed(ref, k):
        return pltpu.make_async_remote_copy(
            ref, ref, csend.at[k], crecv.at[k], device_id={"dp": group + 1 - 2 * core}, device_id_type=MESH
        )

    ups = 0 if shared else 0
    wo_in = copy(wo_hbm.at[half_of(inner)], wov.at[half_of(inner)], sem_in.at[4])

    def up_half_in(c):
        return copy(wu_hbm.at[half_of(d), pl.ds(c * COLS, COLS)], uv.at[c, half_of(d)], sem_w.at[1, c])

    hands = [handed(wov.at[half_of(inner)], ups)] if shared else []
    up_hands = [handed(uv.at[c, half_of(d)], c) for c in range(ups)]

    def k_in(p):
        slot = lax.rem(p, RING)
        return copy(k_hbm.at[pl.ds(p * PAIR, PAIR)], kbuf.at[slot], sem_k.at[slot])

    def v_in(p):
        slot = lax.rem(p, RING)
        return copy(v_hbm.at[pl.ds(p * PAIR, PAIR)], vbuf.at[slot], sem_v.at[slot])

    def gate_in(c):
        return copy(wg_hbm.at[:, pl.ds(pl.multiple_of(c * COLS, COLS), COLS)], gv.at[c], sem_w.at[0, c])

    def up_in(c):
        return copy(wu_hbm.at[:, pl.ds(pl.multiple_of(c * COLS, COLS), COLS)], uv.at[c], sem_w.at[1, c])

    def down_in(j):
        return copy(wd_hbm.at[:, block_of(j)], dv.at[j], sem_d.at[j])

    x_in.start()
    ga_in.start()
    turn_in.start()
    for _, _, c in wq_ins:
        c.start()
    gm_in.start()
    for p in range(RING):
        k_in(p).start()
        v_in(p).start()
    wo_in.start()
    for c in range(ups):
        up_half_in(c).start()

    with jax.named_scope("entry"):
        barrier = pltpu.get_barrier_semaphore()
        for j in range(1, n):
            pl.semaphore_signal(barrier, inc=1, device_id={"tp": peer(j)}, device_id_type=MESH)
        if shared:
            pl.semaphore_signal(barrier, inc=1, device_id={"dp": group + 1 - 2 * core}, device_id_type=MESH)
        pl.semaphore_wait(barrier, n if shared else n - 1)

    def widened(gain):
        g = gain[...].astype(F32)
        return jnp.concatenate([g[i : i + 1] for i in range(d // 128)], 1)

    def norm_rows(parts, gain, r, many):
        wide = [part(r, many).astype(F32) for part in parts]
        total = sum(jnp.sum(w * w, -1, keepdims=True) for w in wide)
        scale = lax.rsqrt(total / d + 1e-6)
        step = d // len(parts)
        for i, w in enumerate(wide):
            at = pl.ds(i * step, step)
            normed[pl.ds(r, many), at] = (w * scale * gain[:, at]).astype(BF16)

    with jax.named_scope("x_wait"):
        x_in.wait()
        ga_in.wait()
    gaf[...] = widened(gav)
    for r in range(0, batch, 16):
        norm_rows([lambda r, many: xv[pl.ds(r, many), :]], gaf, r, 16)
    turn_in.wait()
    for c, size, c_in in wq_ins:
        with jax.named_scope("wq_wait"):
            c_in.wait()
        q_s[:, pl.ds(c, size)] = dot(normed[...], gv[c // COLS, :, pl.ds(0, size)])
    half = HEAD // 2
    lane = lax.broadcasted_iota(jnp.int32, (16, inner), 1)
    first = lax.rem(lane, HEAD) < half
    for r in range(0, batch, 16):
        q = q_s[pl.ds(r, 16), :].astype(BF16).astype(F32)
        other = jnp.where(first, pltpu.roll(q, inner - half, 1), pltpu.roll(q, half, 1))
        q_s[pl.ds(r, 16), :] = q * turnv[pl.ds(0, 1), :] + other * turnv[pl.ds(1, 1), :]

    row = lax.broadcasted_iota(jnp.int32, (rows, inner), 0)
    mine = lax.broadcasted_iota(jnp.int32, (rows, inner), 1) // HEAD == lax.rem(row, heads)

    def scores(p):
        slot = lax.rem(p, RING)
        q = jnp.concatenate(
            [jnp.broadcast_to(q_s[pl.ds(p * PAIR + i, 1), :], (heads, inner)) for i in range(PAIR)], 0
        )
        q = jnp.where(mine, q, 0.0).astype(BF16)
        for i in range(PAIR):
            at = pl.ds(i * heads, heads)
            s_s[at, :] = dot(q, kbuf[slot, i])[i * heads : (i + 1) * heads]

    def attend(p, last):
        v_in(p).wait()
        if not last:
            k_in(p + 1).wait()
        s = s_s[...] * HEAD**-0.5
        e = jnp.exp(s - jnp.max(s, -1, keepdims=True))
        w = (e * (1.0 / jnp.sum(e, -1, keepdims=True))).astype(BF16)
        if not last:
            scores(p + 1)
        slot = lax.rem(p, RING)
        for i in range(PAIR):
            o = dot_t(w, vbuf[slot, i])[i * heads : (i + 1) * heads]
            seen[pl.ds(p * PAIR + i, 1), :] = jnp.sum(
                jnp.where(mine[i * heads : (i + 1) * heads], o, 0.0), 0, keepdims=True
            )

        if not last:
            @pl.when(p + 1 + RING < steps)
            def _():
                k_in(p + 1 + RING).start()

            @pl.when(p + RING < steps)
            def _():
                v_in(p + RING).start()

    order = [2, 1, 3] if n == 4 else list(range(1, n))
    places = order + [0]
    by_two = [places[i : i + 2] for i in range(0, n, 2)]
    parts = [(0, EARLY), (EARLY, batch - EARLY)]

    def to(j, src, dst, sems, k):
        return pltpu.make_async_remote_copy(
            src, dst, sems[0].at[k, j - 1], sems[1].at[k, j - 1], device_id={"tp": peer(j)}, device_id_type=MESH
        )

    def term1(k, j):
        at = pl.ds(*parts[k])
        return to(j, t1.at[j - 1, at], rs1.at[j - 1, at], (send1, recv1), k)

    def state1(k, j):
        at = pl.ds(*parts[k])
        return to(j, hbuf.at[me, at], hbuf.at[me, at], (gsend1, grecv1), k)

    def term2(k, j):
        at = pl.ds(*parts[k])
        return to(j, t2.at[j - 1, at], rs2.at[j - 1, at], (send2, recv2), k)

    def state2(k, j):
        at = pl.ds(*parts[k])
        return to(j, ybuf.at[me, at], ybuf.at[me, at], (gsend2, grecv2), k)

    def late_term(k, j):
        return to(j, tb.at[k], rb.at[k, me], (bsend, brecv), k)

    late_rows = pl.ds(EARLY, batch - EARLY)

    def late_out(k):
        t = dot(seen[late_rows, :].astype(BF16), wov[...])[k * LATE : (k + 1) * LATE].astype(BF16)
        tb[k] = t
        rb[k, me] = t
        for j in order:
            late_term(k, j).start()

    def late_in(k):
        for j in order:
            late_term(k, j).wait_recv()
        total = rb[k, 0].astype(F32)
        for i in range(1, n):
            total = total + rb[k, i].astype(F32)
        at = pl.ds(k * LATE, LATE)
        h = xv[late_rows, :].astype(F32)[k * LATE : (k + 1) * LATE] + total
        hlate[at, :] = h.astype(BF16).astype(F32)

    def late_norm():
        wide = hlate[...]
        scale = lax.rsqrt(jnp.mean(wide * wide, -1, keepdims=True) + 1e-6)
        normed[late_rows, :] = (wide * scale * gmf[...]).astype(BF16)
        hbuf[me, late_rows, :] = hlate[:, block_of(0)].astype(BF16)

    def terms_out(k):
        at = pl.ds(*parts[k])
        a = seen[at, :].astype(BF16)
        for group in by_two:
            found = [dot(a, wov[:, block_of(j)]) for j in group]
            for j, t in zip(group, found):
                if j:
                    t1[j - 1, at, :] = t.astype(BF16)
                else:
                    acc[at, :] = t
            for j in group:
                if j:
                    term1(k, j).start()

    def states_out(k):
        at = pl.ds(*parts[k])
        for j in order:
            term1(k, j).wait_recv()
        total = acc[at, :]
        for j in range(1, n):
            total = total + rs1[j - 1, at, :].astype(F32)
        hbuf[me, at, :] = (xv[at, block_of(0)].astype(F32) + total).astype(BF16)
        for j in order:
            state1(k, j).start()

    def states_in(k):
        for j in order:
            state1(k, j).wait_recv()
        r, many = parts[k]
        for i in range(r, r + many, 16):
            norm_rows([lambda r, many, s=s: hbuf[s, pl.ds(r, many), :] for s in range(n)], gmf, i, 16)

    units = [u for c in range(chunks) for u in ((gate_in(c),) if c < ups else (gate_in(c), up_in(c)))] + [down_in(j) for j in places]
    started = [0]

    def start(many):
        for u in units[started[0] : started[0] + many]:
            u.start(priority=1)
        started[0] += many

    early_steps = EARLY // PAIR
    scope = jax.named_scope

    def body(p, carry):
        if shared:
            @pl.when(p == early_steps // 4)
            def _():
                with scope("hand"):
                    wo_in.wait()
                    for c in range(ups):
                        up_half_in(c).wait()
                    for h in hands + up_hands:
                        h.start()

        @pl.when(p == early_steps)
        def _():
            with scope("terms_a"):
                if not shared:
                    wo_in.wait()
                for h in hands:
                    h.wait_recv()
                terms_out(0)

        @pl.when(p == steps - LATE // PAIR)
        def _():
            with scope("states_a"):
                states_out(0)
            with scope("terms_m"):
                late_out(0)

        attend(p, False)

        @pl.when(p == steps - 1 - RING)
        def _():
            start(4)

        return carry

    with scope("first_scores"):
        k_in(0).wait()
        scores(0)
        k_in(RING).start()
    with scope("attend"):
        lax.fori_loop(0, steps - 1, body, 0)
    with scope("attend_last"):
        start(2)
        attend(steps - 1, True)
        start(2)
    with scope("terms_b"):
        late_out(1)
        start(2)

    def hidden_out(cs, rows):
        at = pl.ds(*rows)
        for c in cs:
            g = dot(normed[at, :], gv[c])
            u = dot(normed[at, :], uv[c])
            hidden[at, pl.ds(c * COLS, COLS)] = (jax.nn.silu(g) * u).astype(BF16)

    def weights_in(cs):
        for c in cs:
            gate_in(c).wait()
            if c < ups:
                up_hands[c].wait_recv()
            else:
                up_in(c).wait()

    former, latter = range(chunks // 2), range(chunks // 2, chunks)
    with scope("norm_a"):
        gm_in.wait()
        gmf[...] = widened(gmv)
        states_in(0)
        for j in order:
            term1(0, j).wait_send()
        late_in(0)
    with scope("weights_wait"):
        weights_in(former)
    with scope("hidden_a"):
        hidden_out(former, parts[0])
        start(n - 2)
    with scope("norm_b"):
        late_in(1)
        late_norm()
    with scope("weights_wait"):
        weights_in(latter)
    with scope("hidden_ab"):
        hidden_out(latter, (0, batch))

    def down_out(k):
        at = pl.ds(*parts[k])
        for group in by_two:
            if k == 0:
                with scope("down_wait"):
                    for j in group:
                        down_in(j).wait()
            with scope("down"):
                found = [dot(hidden[at, :], dv[j]) for j in group]
                for j, t in zip(group, found):
                    if j:
                        t2[j - 1, at, :] = t.astype(BF16)
                    else:
                        acc[at, :] = t
                for j in group:
                    if j:
                        term2(k, j).start()

    down_out(0)
    with scope("hidden_b"):
        hidden_out(former, parts[1])
    down_out(1)
    for k in range(2):
        at = pl.ds(*parts[k])
        with scope("terms2_wait"):
            for j in order:
                term2(k, j).wait_recv()
        total = acc[at, :]
        for j in range(1, n):
            total = total + rs2[j - 1, at, :].astype(F32)
        ybuf[me, at, :] = (hbuf[me, at, :].astype(F32) + total).astype(BF16)
        for j in order:
            state2(k, j).start()
    with scope("states2_wait"):
        for k in range(2):
            at = pl.ds(*parts[k])
            for j in order:
                state2(k, j).wait_recv()
            for i in range(n):
                out[at, pl.ds(i * width, width)] = ybuf[i, at, :]
    for h in hands + up_hands:
        h.wait_send()
    for k in range(2):
        for j in order:
            for c in (late_term, term2, state2):
                c(k, j).wait_send()
            if k == 0:
                state1(k, j).wait_send()


def turns(place, inner):
    half = HEAD // 2
    angle = np.float32(place) * np.float32(THETA) ** (-np.arange(half, dtype=np.float32) / np.float32(half))
    cos, sin = np.cos(angle.astype(np.float32)), np.sin(angle.astype(np.float32))
    one = np.stack([np.concatenate([cos, cos]), np.concatenate([-sin, sin])])
    return np.tile(one, (1, inner // HEAD)).astype(np.float32)


def solution(mesh):
    n = mesh.shape["tp"]
    shared = 2 if mesh.shape["dp"] % 2 == 0 else 0

    def step(x, k_cache, v_cache, gain_a, wq, wo, gain_m, w_gate, w_up, w_down):
        batch, d = x.shape
        places, heads, head = k_cache.shape[1:]
        inner, ff = heads * head, w_gate.shape[1]
        width = d // n
        turn = jnp.asarray(turns(places - 1, inner))

        def rows_first(c):
            return jnp.transpose(c, (0, 2, 3, 1)).reshape(batch, inner, places)

        anywhere = pl.BlockSpec(memory_space=pl.ANY)
        dma = pltpu.SemaphoreType.DMA
        moved = n - 1
        return pl.pallas_call(
            functools.partial(kernel, n, shared),
            name="layer",
            out_shape=pltpu.VMEM((batch, d), BF16),
            in_specs=[anywhere] * 11,
            out_specs=pl.BlockSpec(memory_space=pltpu.VMEM),
            scratch_shapes=[
                pltpu.VMEM((batch, d), BF16),
                pltpu.VMEM((d // 128, 128), BF16),
                pltpu.VMEM((d // 128, 128), BF16),
                pltpu.VMEM((1, d), F32),
                pltpu.VMEM((1, d), F32),
                pltpu.VMEM((2, inner), F32),
                pltpu.VMEM((ff // COLS, d, COLS), BF16),
                pltpu.VMEM((ff // COLS, d, COLS), BF16),
                pltpu.VMEM((n, ff, width), BF16),
                pltpu.VMEM((inner, d), BF16),
                pltpu.VMEM((RING, PAIR, inner, places), BF16),
                pltpu.VMEM((RING, PAIR, inner, places), BF16),
                pltpu.VMEM((batch, inner), F32),
                pltpu.VMEM((PAIR * heads, places), F32),
                pltpu.VMEM((batch, d), BF16),
                pltpu.VMEM((n, batch, width), BF16),
                pltpu.VMEM((batch, ff), BF16),
                pltpu.VMEM((batch, width), F32),
                pltpu.VMEM((moved, batch, width), BF16),
                pltpu.VMEM((moved, EARLY, width), BF16),
                pltpu.VMEM((moved, batch, width), BF16),
                pltpu.VMEM((n, batch, width), BF16),
                pltpu.VMEM((2, LATE, d), BF16),
                pltpu.VMEM((2, n, LATE, d), BF16),
                pltpu.VMEM((2 * LATE, d), F32),
                dma((5,)),
                dma((RING,)),
                dma((RING,)),
                dma((2, ff // COLS)),
                dma((n,)),
            ]
            + [dma((2, moved))] * 10
            + [dma((3,))] * 2,
            compiler_params=pltpu.CompilerParams(
                collective_id=0, has_side_effects=True, vmem_limit_bytes=VMEM_BYTES
            ),
        )(
            x, rows_first(k_cache), rows_first(v_cache), gain_a.reshape(-1, 128), gain_m.reshape(-1, 128), turn,
            wq, wo, w_gate, w_up, w_down,
        )

    states, cache, columns, rows_of = P("dp", None), P("dp", None, "tp", None), P(None, "tp"), P("tp", None)
    return jax.shard_map(
        step,
        mesh=mesh,
        in_specs=(states, cache, cache, P(None), columns, rows_of, P(None), columns, columns, rows_of),
        out_specs=states,
        check_vma=False,
    )
```

```python
import functools

import jax
import jax.numpy as jnp
import numpy as np
from jax import lax
from jax.experimental import pallas as pl
from jax.experimental.pallas import tpu as pltpu
from jax.sharding import PartitionSpec as P

HEAD = 96
THETA = 10000
MESH = pl.DeviceIdType.MESH
F32, BF16 = jnp.float32, jnp.bfloat16
PAIR = 2
RING = 3
COLS = 512
EARLY = 48
LATE = 8
VMEM_BYTES = 66_400_000


def dot(a, b):
    return lax.dot_general(a, b, (((1,), (0,)), ((), ())), preferred_element_type=F32)


def dot_t(a, b):
    return lax.dot_general(a, b, (((1,), (1,)), ((), ())), preferred_element_type=F32)


def kernel(n, shared, x_hbm, k_hbm, v_hbm, ga_hbm, gm_hbm, turn_hbm, wq_hbm, wo_hbm, wg_hbm, wu_hbm, wd_hbm, out,
           xv, gav, gmv, gaf, gmf, turnv, gv, uv, dv, wov, kbuf, vbuf, q_s, s_s, normed, hbuf, hidden,
           acc, t1, rs1, rs2, ybuf, tb, rb, hlate,
           sem_in, sem_k, sem_v, sem_w, sem_d, send1, recv1, gsend1, grecv1, send2, recv2, gsend2, grecv2, bsend, brecv, csend, crecv):
    batch, d = xv.shape
    t2 = t1
    seen = q_s
    width = d // n
    inner = q_s.shape[1]
    heads = inner // HEAD
    rows = PAIR * heads
    steps = batch // PAIR
    chunks = gv.shape[0]
    me = lax.axis_index("tp")

    def peer(j):
        return lax.rem(me + j, n)

    def block_of(j):
        return pl.ds(pl.multiple_of(peer(j) * width, width), width)

    copy = pltpu.make_async_copy
    x_in = copy(x_hbm, xv, sem_in.at[0])
    ga_in = copy(ga_hbm, gav, sem_in.at[1])
    gm_in = copy(gm_hbm, gmv, sem_in.at[2])
    turn_in = copy(turn_hbm, turnv, sem_in.at[3])

    group = lax.axis_index("dp")
    core = lax.rem(group, 2)

    def half_of(many):
        return pl.ds(pl.multiple_of(core * (many // 2), many // 2), many // 2) if shared else pl.ds(0, many)

    def handed(ref, k):
        return pltpu.make_async_remote_copy(
            ref, ref, csend.at[k], crecv.at[k], device_id={"dp": group + 1 - 2 * core}, device_id_type=MESH
        )

    ups = 0 if shared else 0
    wo_in = copy(wo_hbm.at[half_of(inner)], wov.at[half_of(inner)], sem_in.at[4])

    wq_ins, wq_hands = [], []
    for i, c in enumerate(range(0, inner, COLS)):
        size = min(COLS, inner - c)
        to_ref = gv.at[i, half_of(d), pl.ds(0, size)]
        wq_ins.append((c, size, copy(wq_hbm.at[half_of(d), pl.ds(c, size)], to_ref, sem_w.at[0, i])))
        if shared:
            wq_hands.append(handed(to_ref, 1 + i))

    def up_half_in(c):
        return copy(wu_hbm.at[half_of(d), pl.ds(c * COLS, COLS)], uv.at[c, half_of(d)], sem_w.at[1, c])

    hands = [handed(wov.at[half_of(inner)], ups)] if shared else []
    up_hands = [handed(uv.at[c, half_of(d)], c) for c in range(ups)]

    def k_in(p):
        slot = lax.rem(p, RING)
        return copy(k_hbm.at[pl.ds(p * PAIR, PAIR)], kbuf.at[slot], sem_k.at[slot])

    def v_in(p):
        slot = lax.rem(p, RING)
        return copy(v_hbm.at[pl.ds(p * PAIR, PAIR)], vbuf.at[slot], sem_v.at[slot])

    def gate_in(c):
        return copy(wg_hbm.at[:, pl.ds(pl.multiple_of(c * COLS, COLS), COLS)], gv.at[c], sem_w.at[0, c])

    def up_in(c):
        return copy(wu_hbm.at[:, pl.ds(pl.multiple_of(c * COLS, COLS), COLS)], uv.at[c], sem_w.at[1, c])

    def down_in(j):
        return copy(wd_hbm.at[:, block_of(j)], dv.at[j], sem_d.at[j])

    x_in.start()
    ga_in.start()
    turn_in.start()
    for _, _, c in wq_ins:
        c.start()
    gm_in.start()
    for p in range(RING):
        k_in(p).start(priority=1)
        v_in(p).start(priority=1)
    wo_in.start(priority=1)
    for c in range(ups):
        up_half_in(c).start()

    with jax.named_scope("entry"):
        barrier = pltpu.get_barrier_semaphore()
        for j in range(1, n):
            pl.semaphore_signal(barrier, inc=1, device_id={"tp": peer(j)}, device_id_type=MESH)
        if shared:
            pl.semaphore_signal(barrier, inc=1, device_id={"dp": group + 1 - 2 * core}, device_id_type=MESH)
        pl.semaphore_wait(barrier, n if shared else n - 1)

    def widened(gain):
        g = gain[...].astype(F32)
        return jnp.concatenate([g[i : i + 1] for i in range(d // 128)], 1)

    def norm_rows(parts, gain, r, many):
        wide = [part(r, many).astype(F32) for part in parts]
        total = sum(jnp.sum(w * w, -1, keepdims=True) for w in wide)
        scale = lax.rsqrt(total / d + 1e-6)
        step = d // len(parts)
        for i, w in enumerate(wide):
            at = pl.ds(i * step, step)
            normed[pl.ds(r, many), at] = (w * scale * gain[:, at]).astype(BF16)

    for h, (_, _, c_in) in zip(wq_hands, wq_ins):
        c_in.wait()
        h.start()
    with jax.named_scope("x_wait"):
        x_in.wait()
        ga_in.wait()
    gaf[...] = widened(gav)
    for r in range(0, batch, 16):
        norm_rows([lambda r, many: xv[pl.ds(r, many), :]], gaf, r, 16)
    turn_in.wait()
    for i, (c, size, c_in) in enumerate(wq_ins):
        with jax.named_scope("wq_wait"):
            if shared:
                wq_hands[i].wait_recv()
            else:
                c_in.wait()
        q_s[:, pl.ds(c, size)] = dot(normed[...], gv[c // COLS, :, pl.ds(0, size)])
    half = HEAD // 2
    lane = lax.broadcasted_iota(jnp.int32, (16, inner), 1)
    first = lax.rem(lane, HEAD) < half
    for r in range(0, batch, 16):
        q = q_s[pl.ds(r, 16), :].astype(BF16).astype(F32)
        other = jnp.where(first, pltpu.roll(q, inner - half, 1), pltpu.roll(q, half, 1))
        q_s[pl.ds(r, 16), :] = q * turnv[pl.ds(0, 1), :] + other * turnv[pl.ds(1, 1), :]

    row = lax.broadcasted_iota(jnp.int32, (rows, inner), 0)
    mine = lax.broadcasted_iota(jnp.int32, (rows, inner), 1) // HEAD == lax.rem(row, heads)

    def scores(p):
        slot = lax.rem(p, RING)
        q = jnp.concatenate(
            [jnp.broadcast_to(q_s[pl.ds(p * PAIR + i, 1), :], (heads, inner)) for i in range(PAIR)], 0
        )
        q = jnp.where(mine, q, 0.0).astype(BF16)
        for i in range(PAIR):
            at = pl.ds(i * heads, heads)
            s_s[at, :] = dot(q, kbuf[slot, i])[i * heads : (i + 1) * heads]

    def attend(p, last):
        v_in(p).wait()
        if not last:
            k_in(p + 1).wait()
        s = s_s[...] * HEAD**-0.5
        e = jnp.exp(s - jnp.max(s, -1, keepdims=True))
        w = (e * (1.0 / jnp.sum(e, -1, keepdims=True))).astype(BF16)
        if not last:
            scores(p + 1)
        slot = lax.rem(p, RING)
        for i in range(PAIR):
            o = dot_t(w, vbuf[slot, i])[i * heads : (i + 1) * heads]
            seen[pl.ds(p * PAIR + i, 1), :] = jnp.sum(
                jnp.where(mine[i * heads : (i + 1) * heads], o, 0.0), 0, keepdims=True
            )

        if not last:
            @pl.when(p + 1 + RING < steps)
            def _():
                k_in(p + 1 + RING).start()

            @pl.when(p + RING < steps)
            def _():
                v_in(p + RING).start()

    order = [2, 1, 3] if n == 4 else list(range(1, n))
    places = order + [0]
    by_two = [places[i : i + 2] for i in range(0, n, 2)]
    parts = [(0, EARLY), (EARLY, batch - EARLY)]

    def to(j, src, dst, sems, k):
        return pltpu.make_async_remote_copy(
            src, dst, sems[0].at[k, j - 1], sems[1].at[k, j - 1], device_id={"tp": peer(j)}, device_id_type=MESH
        )

    def term1(k, j):
        at = pl.ds(*parts[k])
        return to(j, t1.at[j - 1, at], rs1.at[j - 1, at], (send1, recv1), k)

    def state1(k, j):
        at = pl.ds(*parts[k])
        return to(j, hbuf.at[me, at], hbuf.at[me, at], (gsend1, grecv1), k)

    def term2(k, j):
        at = pl.ds(*parts[k])
        return to(j, t2.at[j - 1, at], rs2.at[j - 1, at], (send2, recv2), k)

    def state2(k, j):
        at = pl.ds(*parts[k])
        return to(j, ybuf.at[me, at], ybuf.at[me, at], (gsend2, grecv2), k)

    def late_term(k, j):
        return to(j, tb.at[k], rb.at[k, me], (bsend, brecv), k)

    late_rows = pl.ds(EARLY, batch - EARLY)

    def late_out(k):
        t = dot(seen[late_rows, :].astype(BF16), wov[...])[k * LATE : (k + 1) * LATE].astype(BF16)
        tb[k] = t
        rb[k, me] = t
        for j in order:
            late_term(k, j).start()

    def late_in(k):
        for j in order:
            late_term(k, j).wait_recv()
        total = rb[k, 0].astype(F32)
        for i in range(1, n):
            total = total + rb[k, i].astype(F32)
        at = pl.ds(k * LATE, LATE)
        h = xv[late_rows, :].astype(F32)[k * LATE : (k + 1) * LATE] + total
        hlate[at, :] = h.astype(BF16).astype(F32)

    def late_norm():
        wide = hlate[...]
        scale = lax.rsqrt(jnp.mean(wide * wide, -1, keepdims=True) + 1e-6)
        normed[late_rows, :] = (wide * scale * gmf[...]).astype(BF16)
        hbuf[me, late_rows, :] = hlate[:, block_of(0)].astype(BF16)

    def terms_out(k):
        at = pl.ds(*parts[k])
        a = seen[at, :].astype(BF16)
        for group in by_two:
            found = [dot(a, wov[:, block_of(j)]) for j in group]
            for j, t in zip(group, found):
                if j:
                    t1[j - 1, at, :] = t.astype(BF16)
                else:
                    acc[at, :] = t
            for j in group:
                if j:
                    term1(k, j).start()

    def states_out(k):
        at = pl.ds(*parts[k])
        for j in order:
            term1(k, j).wait_recv()
        total = acc[at, :]
        for j in range(1, n):
            total = total + rs1[j - 1, at, :].astype(F32)
        hbuf[me, at, :] = (xv[at, block_of(0)].astype(F32) + total).astype(BF16)
        for j in order:
            state1(k, j).start()

    def states_in(k):
        for j in order:
            state1(k, j).wait_recv()
        r, many = parts[k]
        for i in range(r, r + many, 16):
            norm_rows([lambda r, many, s=s: hbuf[s, pl.ds(r, many), :] for s in range(n)], gmf, i, 16)

    units = [u for c in range(chunks) for u in ((gate_in(c),) if c < ups else (gate_in(c), up_in(c)))] + [down_in(j) for j in places]
    started = [0]

    def start(many):
        for u in units[started[0] : started[0] + many]:
            u.start(priority=1)
        started[0] += many

    early_steps = EARLY // PAIR
    scope = jax.named_scope

    def body(p, carry):
        if shared:
            @pl.when(p == early_steps // 4)
            def _():
                with scope("hand"):
                    for h in wq_hands:
                        h.wait_send()
                    wo_in.wait()
                    for c in range(ups):
                        up_half_in(c).wait()
                    for h in hands + up_hands:
                        h.start()

        @pl.when(p == early_steps)
        def _():
            with scope("terms_a"):
                if not shared:
                    wo_in.wait()
                for h in hands:
                    h.wait_recv()
                terms_out(0)

        @pl.when(p == steps - LATE // PAIR)
        def _():
            with scope("states_a"):
                states_out(0)
            with scope("terms_m"):
                late_out(0)

        attend(p, False)

        @pl.when(p == steps - 1 - RING)
        def _():
            start(4)

        return carry

    with scope("first_scores"):
        k_in(0).wait()
        scores(0)
        k_in(RING).start()
    with scope("attend"):
        lax.fori_loop(0, steps - 1, body, 0)
    with scope("attend_last"):
        start(2)
        attend(steps - 1, True)
        start(2)
    with scope("terms_b"):
        late_out(1)
        start(2)

    def hidden_out(cs, rows):
        at = pl.ds(*rows)
        for c in cs:
            g = dot(normed[at, :], gv[c])
            u = dot(normed[at, :], uv[c])
            hidden[at, pl.ds(c * COLS, COLS)] = (jax.nn.silu(g) * u).astype(BF16)

    def weights_in(cs):
        for c in cs:
            gate_in(c).wait()
            if c < ups:
                up_hands[c].wait_recv()
            else:
                up_in(c).wait()

    former, latter = range(chunks // 2), range(chunks // 2, chunks)
    with scope("norm_a"):
        gm_in.wait()
        gmf[...] = widened(gmv)
        states_in(0)
        for j in order:
            term1(0, j).wait_send()
        late_in(0)
    with scope("weights_wait"):
        weights_in(former)
    with scope("hidden_a"):
        hidden_out(former, parts[0])
        start(n - 2)
    with scope("norm_b"):
        late_in(1)
        late_norm()
    with scope("weights_wait"):
        weights_in(latter)
    with scope("hidden_ab"):
        hidden_out(latter, (0, batch))

    def down_out(k):
        at = pl.ds(*parts[k])
        for group in by_two:
            if k == 0:
                with scope("down_wait"):
                    for j in group:
                        down_in(j).wait()
            with scope("down"):
                found = [dot(hidden[at, :], dv[j]) for j in group]
                for j, t in zip(group, found):
                    if j:
                        t2[j - 1, at, :] = t.astype(BF16)
                    else:
                        acc[at, :] = t
                for j in group:
                    if j:
                        term2(k, j).start()

    down_out(0)
    with scope("hidden_b"):
        hidden_out(former, parts[1])
    down_out(1)
    for k in range(2):
        at = pl.ds(*parts[k])
        with scope("terms2_wait"):
            for j in order:
                term2(k, j).wait_recv()
        total = acc[at, :]
        for j in range(1, n):
            total = total + rs2[j - 1, at, :].astype(F32)
        ybuf[me, at, :] = (hbuf[me, at, :].astype(F32) + total).astype(BF16)
        for j in order:
            state2(k, j).start()
    with scope("states2_wait"):
        for k in range(2):
            at = pl.ds(*parts[k])
            for j in order:
                state2(k, j).wait_recv()
            for i in range(n):
                out[at, pl.ds(i * width, width)] = ybuf[i, at, :]
    for h in hands + up_hands:
        h.wait_send()
    for k in range(2):
        for j in order:
            for c in (late_term, term2, state2):
                c(k, j).wait_send()
            if k == 0:
                state1(k, j).wait_send()


def turns(place, inner):
    half = HEAD // 2
    angle = np.float32(place) * np.float32(THETA) ** (-np.arange(half, dtype=np.float32) / np.float32(half))
    cos, sin = np.cos(angle.astype(np.float32)), np.sin(angle.astype(np.float32))
    one = np.stack([np.concatenate([cos, cos]), np.concatenate([-sin, sin])])
    return np.tile(one, (1, inner // HEAD)).astype(np.float32)


def solution(mesh):
    n = mesh.shape["tp"]
    shared = 2 if mesh.shape["dp"] % 2 == 0 else 0

    def step(x, k_cache, v_cache, gain_a, wq, wo, gain_m, w_gate, w_up, w_down):
        batch, d = x.shape
        places, heads, head = k_cache.shape[1:]
        inner, ff = heads * head, w_gate.shape[1]
        width = d // n
        turn = jnp.asarray(turns(places - 1, inner))

        def rows_first(c):
            return jnp.transpose(c, (0, 2, 3, 1)).reshape(batch, inner, places)

        anywhere = pl.BlockSpec(memory_space=pl.ANY)
        dma = pltpu.SemaphoreType.DMA
        moved = n - 1
        return pl.pallas_call(
            functools.partial(kernel, n, shared),
            name="layer",
            out_shape=pltpu.VMEM((batch, d), BF16),
            in_specs=[anywhere] * 11,
            out_specs=pl.BlockSpec(memory_space=pltpu.VMEM),
            scratch_shapes=[
                pltpu.VMEM((batch, d), BF16),
                pltpu.VMEM((d // 128, 128), BF16),
                pltpu.VMEM((d // 128, 128), BF16),
                pltpu.VMEM((1, d), F32),
                pltpu.VMEM((1, d), F32),
                pltpu.VMEM((2, inner), F32),
                pltpu.VMEM((ff // COLS, d, COLS), BF16),
                pltpu.VMEM((ff // COLS, d, COLS), BF16),
                pltpu.VMEM((n, ff, width), BF16),
                pltpu.VMEM((inner, d), BF16),
                pltpu.VMEM((RING, PAIR, inner, places), BF16),
                pltpu.VMEM((RING, PAIR, inner, places), BF16),
                pltpu.VMEM((batch, inner), F32),
                pltpu.VMEM((PAIR * heads, places), F32),
                pltpu.VMEM((batch, d), BF16),
                pltpu.VMEM((n, batch, width), BF16),
                pltpu.VMEM((batch, ff), BF16),
                pltpu.VMEM((batch, width), F32),
                pltpu.VMEM((moved, batch, width), BF16),
                pltpu.VMEM((moved, EARLY, width), BF16),
                pltpu.VMEM((moved, batch, width), BF16),
                pltpu.VMEM((n, batch, width), BF16),
                pltpu.VMEM((2, LATE, d), BF16),
                pltpu.VMEM((2, n, LATE, d), BF16),
                pltpu.VMEM((2 * LATE, d), F32),
                dma((5,)),
                dma((RING,)),
                dma((RING,)),
                dma((2, ff // COLS)),
                dma((n,)),
            ]
            + [dma((2, moved))] * 10
            + [dma((3,))] * 2,
            compiler_params=pltpu.CompilerParams(
                collective_id=0, has_side_effects=True, vmem_limit_bytes=VMEM_BYTES
            ),
        )(
            x, rows_first(k_cache), rows_first(v_cache), gain_a.reshape(-1, 128), gain_m.reshape(-1, 128), turn,
            wq, wo, w_gate, w_up, w_down,
        )

    states, cache, columns, rows_of = P("dp", None), P("dp", None, "tp", None), P(None, "tp"), P("tp", None)
    return jax.shard_map(
        step,
        mesh=mesh,
        in_specs=(states, cache, cache, P(None), columns, rows_of, P(None), columns, columns, rows_of),
        out_specs=states,
        check_vma=False,
    )
```
